8 devices in a mesh: dp: 1 (over z), tp: 2 (over y), cp: 4 (over x, core).
Axes of the slice: x: 2, y: 2, z: 1, core: 2. Of those that a mesh axis runs over, the one named last changes fastest.
Arguments:
- x: bfloat16 [4096, 6144], P(('dp', 'cp'))
- k_cache: bfloat16 [1024, 8, 128], P(('dp', 'cp'), 'tp')
- v_cache: bfloat16 [1024, 8, 128], P(('dp', 'cp'), 'tp')
- rope_table: float32 [4096, 64], P(('dp', 'cp'))
- norm_gain: bfloat16 [6144], replicated
- w_qkv: bfloat16 [6144, 8192], P(None, 'tp')
- b_qkv: bfloat16 [8192], P('tp')
- w_out: bfloat16 [6144, 6144], P('tp')
Outputs:
- output 1: bfloat16 [4096, 6144], P(('dp', 'cp'))
- output 2: bfloat16 [4096, 8, 128], P(('dp', 'cp'), 'tp')
- output 3: bfloat16 [4096, 8, 128], P(('dp', 'cp'), 'tp')
All inputs are finite; a program needn't handle non-finite values.
Results may differ from the reference program's by a relative error of at most 0.0044295.
Values are sent between devices in bfloat16 or wider.
A program may use at most 1 GiB of HBM per device.

```python
import math
import jax
import jax.numpy as jnp
from jax import lax

D = 6144
HEADS = 48
KV_HEADS = 8
HEAD = 128
NEW_TOKENS = 4096
PREFIX = 1024
EPS = 1.5625e-07
MASK_VALUE = -1e30
GROUP = HEADS // KV_HEADS
QKV_WIDTH = (HEADS + 2 * KV_HEADS) * HEAD
PAIR_COUNT = HEAD // 4
QUERY_BLOCK = math.gcd(NEW_TOKENS, 128)
KEY_BLOCK = math.gcd(PREFIX + NEW_TOKENS, 512)


def setup_inputs(seed: int = 0, part: int = 0) -> dict:
    part_keys = jax.random.split(jax.random.fold_in(jax.random.key(seed), part), 4)
    shared_keys = jax.random.split(jax.random.key(seed + 1), 4)
    x = jax.random.normal(part_keys[0], (NEW_TOKENS, D), jnp.float32)
    k_cache = 1.6 * jax.random.normal(part_keys[1], (PREFIX, KV_HEADS, HEAD), jnp.float32)
    v_cache = 1.6 * jax.random.normal(part_keys[2], (PREFIX, KV_HEADS, HEAD), jnp.float32)
    log_ratio = jax.random.uniform(part_keys[3], (), jnp.float32, math.log(100.0), math.log(10000.0))
    rope_base = 10000.0 * jnp.exp(log_ratio)
    inv_freq = rope_base ** (-jnp.arange(PAIR_COUNT, dtype=jnp.float32) / PAIR_COUNT)
    positions = (PREFIX + jnp.arange(NEW_TOKENS)).astype(jnp.float32)
    angles = positions[:, None] * inv_freq[None, :]
    rope_table = jnp.concatenate([jnp.cos(angles), jnp.sin(angles)], axis=1)
    norm_gain = 1.0 + 0.3 * jax.random.normal(shared_keys[0], (D,), jnp.float32)
    w_qkv = jax.random.normal(shared_keys[1], (D, QKV_WIDTH), jnp.float32) * (1.5 / math.sqrt(D))
    b_qkv = 0.5 * jax.random.normal(shared_keys[2], (QKV_WIDTH,), jnp.float32)
    w_out = jax.random.normal(shared_keys[3], (HEADS * HEAD, D), jnp.float32) / math.sqrt(HEADS * HEAD)
    return dict(x=x.astype(jnp.bfloat16), k_cache=k_cache.astype(jnp.bfloat16), v_cache=v_cache.astype(jnp.bfloat16), rope_table=rope_table.astype(jnp.float32), norm_gain=norm_gain.astype(jnp.bfloat16), w_qkv=w_qkv.astype(jnp.bfloat16), b_qkv=b_qkv.astype(jnp.bfloat16), w_out=w_out.astype(jnp.bfloat16))


def apply_rotary(vals, cos_t, sin_t):
    pair_count = cos_t.shape[-1]
    lead_shape = vals.shape[:-1]
    paired = vals[..., :2 * pair_count].reshape(lead_shape + (pair_count, 2))
    even_part = paired[..., 0]
    odd_part = paired[..., 1]
    turned = jnp.stack([even_part * cos_t - odd_part * sin_t, odd_part * cos_t + even_part * sin_t], axis=-1)
    return jnp.concatenate([turned.reshape(lead_shape + (2 * pair_count,)), vals[..., 2 * pair_count:]], axis=-1)


def reference(x, k_cache, v_cache, rope_table, norm_gain, w_qkv, b_qkv, w_out):
    x_f32 = x.astype(jnp.float32)
    inv_rms = lax.rsqrt(jnp.mean(x_f32 * x_f32, axis=-1, keepdims=True) + EPS)
    hidden = (x_f32 * inv_rms * norm_gain.astype(jnp.float32)).astype(jnp.bfloat16)
    qkv_all = jnp.dot(hidden, w_qkv, preferred_element_type=jnp.float32) + b_qkv.astype(jnp.float32)
    qkv_all = qkv_all.reshape(NEW_TOKENS, KV_HEADS, GROUP + 2, HEAD)
    cos_t = rope_table[:, :PAIR_COUNT]
    sin_t = rope_table[:, PAIR_COUNT:]
    queries = apply_rotary(qkv_all[:, :, :GROUP], cos_t[:, None, None], sin_t[:, None, None]).astype(jnp.bfloat16)
    new_k = apply_rotary(qkv_all[:, :, GROUP], cos_t[:, None], sin_t[:, None]).astype(jnp.bfloat16)
    new_v = qkv_all[:, :, GROUP + 1].astype(jnp.bfloat16)
    key_count = PREFIX + NEW_TOKENS
    key_blocks = key_count // KEY_BLOCK
    keys_all = jnp.concatenate([k_cache, new_k], axis=0).reshape(key_blocks, KEY_BLOCK, KV_HEADS, HEAD)
    vals_all = jnp.concatenate([v_cache, new_v], axis=0).reshape(key_blocks, KEY_BLOCK, KV_HEADS, HEAD)
    key_pos = jnp.arange(key_count).reshape(key_blocks, KEY_BLOCK)
    q_blocks = queries.reshape(NEW_TOKENS // QUERY_BLOCK, QUERY_BLOCK, KV_HEADS, GROUP, HEAD)
    q_pos = (PREFIX + jnp.arange(NEW_TOKENS)).reshape(NEW_TOKENS // QUERY_BLOCK, QUERY_BLOCK)
    scale = HEAD ** -0.5

    def query_block(block):
        q_vals, q_at = block
        q_f32 = q_vals.astype(jnp.float32)

        def key_step(carry, kv_block):
            run_max, run_sum, weighted = carry
            k_vals, v_vals, k_at = kv_block
            scores = jnp.einsum('qngd,knd->qngk', q_f32, k_vals.astype(jnp.float32)) * scale
            visible = (k_at[None, :] <= q_at[:, None])[:, None, None, :]
            scores = jnp.where(visible, scores, MASK_VALUE)
            new_max = jnp.maximum(run_max, scores.max(axis=-1))
            rescale = jnp.exp(run_max - new_max)
            probs = jnp.exp(scores - new_max[..., None])
            run_sum = run_sum * rescale + probs.sum(axis=-1)
            weighted = weighted * rescale[..., None] + jnp.einsum('qngk,knd->qngd', probs.astype(jnp.bfloat16).astype(jnp.float32), v_vals.astype(jnp.float32))
            return (new_max, run_sum, weighted), None

        start_carry = (jnp.full((QUERY_BLOCK, KV_HEADS, GROUP), MASK_VALUE, jnp.float32), jnp.zeros((QUERY_BLOCK, KV_HEADS, GROUP), jnp.float32), jnp.zeros((QUERY_BLOCK, KV_HEADS, GROUP, HEAD), jnp.float32))
        (run_max, run_sum, weighted), _ = lax.scan(key_step, start_carry, (keys_all, vals_all, key_pos))
        return weighted / run_sum[..., None]

    attn = lax.map(query_block, (q_blocks, q_pos))
    attn = attn.reshape(NEW_TOKENS, HEADS * HEAD).astype(jnp.bfloat16)
    y = (x_f32 + jnp.dot(attn, w_out, preferred_element_type=jnp.float32)).astype(jnp.bfloat16)
    return y, new_k, new_v
```

```python
import functools

import jax
import jax.numpy as jnp
import numpy as np
from jax import lax
from jax.experimental import pallas as pl
from jax.experimental.pallas import tpu as pltpu
from jax.sharding import PartitionSpec as P


EPS = 1.5625e-07
MASK_VALUE = -1e30
F32 = jnp.float32
BF16 = jnp.bfloat16
LOG2E = 1.4426950408889634
HD = 128
VLIM = 60 * 1024 * 1024


def cost(flops, nbytes):
    return pl.CostEstimate(flops=int(flops), bytes_accessed=int(nbytes), transcendentals=0)


def dot(a, b):
    return jnp.dot(a, b, preferred_element_type=F32)


def norm_kernel(x_ref, g_ref, h_ref):
    x = x_ref[...].astype(F32)
    inv = lax.rsqrt(jnp.mean(x * x, axis=-1, keepdims=True) + EPS)
    h_ref[...] = (x * inv * g_ref[...].astype(F32)).astype(BF16)


def norm(x, g):
    rows, d = x.shape
    rb = 128
    return pl.pallas_call(
        norm_kernel,
        grid=(rows // rb,),
        in_specs=[pl.BlockSpec((rb, d), lambda i: (i, 0)), pl.BlockSpec((1, d), lambda i: (0, 0))],
        out_specs=pl.BlockSpec((rb, d), lambda i: (i, 0)),
        out_shape=jax.ShapeDtypeStruct((rows, d), BF16),
        cost_estimate=cost(rows * d * 80, rows * d * 4),
        name="norm",
    )(x, g.reshape(1, d))


def rotate(v, cos_e, sin_e):
    lane = lax.broadcasted_iota(jnp.int32, v.shape, 1)
    swapped = jnp.where(lane % 2 == 0, pltpu.roll(v, HD - 1, 1), pltpu.roll(v, 1, 1))
    return jnp.where(lane < HD // 2, v * cos_e + swapped * sin_e, v)


MB = 512


def kv_kernel(h_ref, w_ref, b_ref, c_ref, s_ref, k_ref, v_ref, vt_ref):
    bias = b_ref[0].astype(F32)

    @pl.loop(0, h_ref.shape[0] // MB)
    def _(m):
        r = pl.ds(pl.multiple_of(m * MB, MB), MB)
        a = dot(h_ref[r, :], w_ref[...]) + bias
        k_ref[r, :] = rotate(a[:, :HD], c_ref[r, :], s_ref[r, :]).astype(BF16)
        v = a[:, HD:].astype(BF16)
        v_ref[r, :] = v
        vt_ref[:, r] = v.T


def q_kernel(h_ref, w_ref, b_ref, c_ref, s_ref, q_ref):
    bias = b_ref[0].astype(F32)

    @pl.loop(0, h_ref.shape[0] // MB)
    def _(m):
        r = pl.ds(pl.multiple_of(m * MB, MB), MB)
        a = dot(h_ref[r, :], w_ref[...]) + bias
        q_ref[r, :HD] = rotate(a[:, :HD], c_ref[r, :], s_ref[r, :]).astype(BF16)
        q_ref[r, HD:] = rotate(a[:, HD:], c_ref[r, :], s_ref[r, :]).astype(BF16)


def proj_specs(rows, d, col):
    whole = lambda i: (0, 0)
    return [
        pl.BlockSpec((rows, d), whole),
        pl.BlockSpec((d, 2 * HD), lambda i: (0, col(i))),
        pl.BlockSpec((1, 1, 2 * HD), lambda i: (col(i), 0, 0)),
        pl.BlockSpec((rows, HD), whole),
        pl.BlockSpec((rows, HD), whole),
    ]


def project_kv(h, w, b, ce, se, groups):
    rows, d = h.shape
    per = w.shape[1] // (2 * HD * groups)
    col = lambda i: i * per + per - 1
    return pl.pallas_call(
        kv_kernel,
        grid=(groups,),
        in_specs=proj_specs(rows, d, col),
        out_specs=[
            pl.BlockSpec((rows, HD), lambda i: (0, i)),
            pl.BlockSpec((rows, HD), lambda i: (0, i)),
            pl.BlockSpec((HD, rows), lambda i: (i, 0)),
        ],
        out_shape=[
            jax.ShapeDtypeStruct((rows, groups * HD), BF16),
            jax.ShapeDtypeStruct((rows, groups * HD), BF16),
            jax.ShapeDtypeStruct((groups * HD, rows), BF16),
        ],
        compiler_params=pltpu.CompilerParams(vmem_limit_bytes=VLIM),
        cost_estimate=cost(2 * rows * d * groups * 2 * HD, d * groups * 4 * HD + rows * d * 2),
        name="project_kv",
    )(h, w, b, ce, se)


def project_q(h, w, b, ce, se, groups):
    rows, d = h.shape
    per = w.shape[1] // (2 * HD * groups)
    nq = per - 1
    col = lambda i: (i // nq) * per + i % nq
    return pl.pallas_call(
        q_kernel,
        grid=(groups * nq,),
        in_specs=proj_specs(rows, d, col),
        out_specs=pl.BlockSpec((rows, 2 * HD), lambda i: (0, i)),
        out_shape=jax.ShapeDtypeStruct((rows, groups * nq * 2 * HD), BF16),
        compiler_params=pltpu.CompilerParams(vmem_limit_bytes=VLIM),
        cost_estimate=cost(2 * rows * d * groups * nq * 2 * HD, d * groups * nq * 4 * HD + rows * d * 2),
        name="project_q",
    )(h, w, b, ce, se)


QB = 256
KB = 512


def attn_kernel(chunk, group, tok, me_ref, q_ref, kc, vc, ko, vo, ks, vs, kx, vx, kz, vz,
                o_ref, kbuf, vbuf, qt, acc, mrun, lrun, sem):
    g = pl.program_id(0)
    groups = kbuf.shape[0]
    me = me_ref[0]
    pieces = [(None, kc, vc), (0, ko, vo), (1, ks, vs), (2, kx, vx), (3, kz, vz)]

    def each_copy(gg, act):
        for rel, kp, vp in pieces:
            n = kp.shape[0]
            src = None if rel is None else lax.bitwise_xor(me, rel)
            at = 0 if rel is None else pl.multiple_of(kc.shape[0] + src * tok, tok)

            def go(kp=kp, vp=vp, n=n, at=at):
                act(pltpu.make_async_copy(kp.at[:, pl.ds(gg * HD, HD)], kbuf.at[gg, pl.ds(at, n), :], sem.at[gg]))
                act(pltpu.make_async_copy(vp.at[pl.ds(gg * HD, HD), :], vbuf.at[gg, :, pl.ds(at, n)], sem.at[gg]))

            if rel in (None, 0):
                go()
            else:
                pl.when(src < me)(go)

    @pl.when(g == 0)
    def _():
        for gg in range(groups):
            each_copy(gg, lambda c: c.start())

    for h in range(group):
        qt[h] = q_ref[:, h * HD:(h + 1) * HD].T
    acc[...] = jnp.zeros_like(acc)
    lrun[...] = jnp.zeros_like(lrun)
    mrun[...] = jnp.full_like(mrun, MASK_VALUE)

    for gg in range(groups):
        @pl.when(g == gg)
        def _(gg=gg):
            each_copy(gg, lambda c: c.wait())

    conv = LOG2E * HD ** -0.5

    def step(kb, mask):
        k = kbuf[g, pl.ds(pl.multiple_of(kb * KB, KB), KB), :]
        vt = vbuf[g, :, pl.ds(pl.multiple_of(kb * KB, KB), KB)]
        for h in range(group):
            s = dot(k, qt[h])
            if mask is not None:
                s = jnp.where(mask, s, MASK_VALUE)
            m_old = mrun[h]
            m_new = jnp.maximum(m_old, jnp.max(s, axis=0, keepdims=True))
            p = jnp.exp2(s * conv - m_new * conv)
            alpha = jnp.exp2((m_old - m_new) * conv)
            mrun[h] = m_new
            lrun[h] = lrun[h] * alpha + p.reshape(KB // 8, 8, QB).sum(axis=0)
            acc[h] = acc[h] * alpha + dot(vt, p.astype(BF16))

    first = kc.shape[0] + me * tok + chunk * QB
    nfull = first // KB

    @pl.loop(0, nfull)
    def _(kb):
        step(kb, None)

    off = (kc.shape[0] + chunk * QB) % KB
    key = lax.broadcasted_iota(jnp.int32, (KB, QB), 0)
    row = lax.broadcasted_iota(jnp.int32, (KB, QB), 1)
    step(nfull, key <= row + off)

    for h in range(group):
        total = jnp.sum(lrun[h], axis=0, keepdims=True)
        o_ref[:, h * HD:(h + 1) * HD] = (acc[h] / total).T.astype(BF16)


def attend(chunk, me, q, pieces, group):
    tok, width = q.shape
    groups = width // (group * HD)
    ncache = pieces[0].shape[0]
    total = ncache + 4 * tok
    anyspec = pl.BlockSpec(memory_space=pl.ANY)
    return pl.pallas_call(
        functools.partial(attn_kernel, chunk, group, tok),
        grid_spec=pltpu.PrefetchScalarGridSpec(
            num_scalar_prefetch=1,
            grid=(groups,),
            in_specs=[pl.BlockSpec((QB, group * HD), lambda g, me: (chunk, g))] + [anyspec] * 10,
            out_specs=pl.BlockSpec((QB, group * HD), lambda g, me: (0, g)),
            scratch_shapes=[
                pltpu.VMEM((groups, total, HD), BF16),
                pltpu.VMEM((groups, HD, total), BF16),
                pltpu.VMEM((group, HD, QB), BF16),
                pltpu.VMEM((group, HD, QB), F32),
                pltpu.VMEM((group, 1, QB), F32),
                pltpu.VMEM((group, 8, QB), F32),
                pltpu.SemaphoreType.DMA((groups,)),
            ],
        ),
        out_shape=jax.ShapeDtypeStruct((QB, width), BF16),
        compiler_params=pltpu.CompilerParams(vmem_limit_bytes=VLIM),
        cost_estimate=cost(40e9, 12e6),
    )(me, q, *pieces)


def own_kernel(nchunk, x_ref, w_ref, *refs):
    chunks, (y_ref, obuf, sem) = refs[:nchunk], refs[nchunk:]
    rows = chunks[0].shape[0]

    @pl.when(pl.program_id(0) == 0)
    def _():
        copies = [pltpu.make_async_copy(c, obuf.at[pl.ds(i * rows, rows), :], sem.at[i]) for i, c in enumerate(chunks)]
        for c in copies:
            c.start()
        for c in copies:
            c.wait()

    @pl.loop(0, obuf.shape[0] // MB)
    def _(m):
        r = pl.ds(pl.multiple_of(m * MB, MB), MB)
        y_ref[r, :] = x_ref[r, :].astype(F32) + dot(obuf[r, :], w_ref[...])


def own_part(x, w, chunks):
    rows, d = x.shape
    inner = w.shape[0]
    nb = 512
    return pl.pallas_call(
        functools.partial(own_kernel, len(chunks)),
        grid=(d // nb,),
        in_specs=[
            pl.BlockSpec((rows, nb), lambda i: (0, i)),
            pl.BlockSpec((inner, nb), lambda i: (0, i)),
        ] + [pl.BlockSpec(memory_space=pl.ANY)] * len(chunks),
        out_specs=pl.BlockSpec((rows, nb), lambda i: (0, i)),
        out_shape=jax.ShapeDtypeStruct((rows, d), F32),
        scratch_shapes=[pltpu.VMEM((rows, inner), BF16), pltpu.SemaphoreType.DMA((len(chunks),))],
        compiler_params=pltpu.CompilerParams(vmem_limit_bytes=VLIM),
        cost_estimate=cost(2 * rows * inner * d, rows * d * 6 + inner * d * 2),
        name="own_part",
    )(x, w, *chunks)


def other_kernel(nper, me_ref, o_ref, a_ref, *refs):
    me = me_ref[0]
    ws, y_ref = refs[:4 * nper], refs[-1]
    wr = ws[0].shape[0]
    total = a_ref[...]
    for i in range(4 * nper):
        quarter = lax.bitwise_xor(me, i // nper)
        at = pl.multiple_of(quarter * (nper * wr) + (i % nper) * wr, wr)
        total = total + dot(o_ref[:, pl.ds(at, wr)], ws[i][...])
    y_ref[...] = total.astype(BF16)


def other_part(chunk, me, o, partial, ws, y):
    rows = o.shape[0]
    d = partial.shape[1]
    nb = 512
    wr = ws[0].shape[0]
    extra = [] if y is None else [y]
    return pl.pallas_call(
        functools.partial(other_kernel, len(ws) // 4),
        grid_spec=pltpu.PrefetchScalarGridSpec(
            num_scalar_prefetch=1,
            grid=(d // nb,),
            in_specs=[
                pl.BlockSpec(o.shape, lambda i, me: (0, 0)),
                pl.BlockSpec((rows, nb), lambda i, me: (chunk, i)),
            ] + [pl.BlockSpec((wr, nb), lambda i, me: (0, i))] * len(ws)
            + [pl.BlockSpec(memory_space=pl.ANY)] * len(extra),
            out_specs=pl.BlockSpec((rows, nb), lambda i, me: (chunk, i)),
        ),
        out_shape=jax.ShapeDtypeStruct(partial.shape, BF16),
        input_output_aliases={} if y is None else {3 + len(ws): 0},
        compiler_params=pltpu.CompilerParams(vmem_limit_bytes=VLIM),
        cost_estimate=cost(2 * rows * wr * len(ws) * d, rows * d * 6 + wr * len(ws) * d * 2),
    )(me, o, partial, *ws, *extra)


def cp_send(v, rel):
    return lax.ppermute(v, 'cp', [(i, i ^ rel) for i in range(4)])


def tp_send(v):
    return lax.ppermute(v, 'tp', [(0, 1), (1, 0)])


def spread_matrices(half, hd):
    out = np.zeros((2 * half, 2 * hd), np.float32)
    for lane in range(2 * half):
        out[lane // 2, lane] = 1.0
        out[half + lane // 2, hd + lane] = 1.0 if lane % 2 else -1.0
    return out


def block(x, k_cache, v_cache, rope_table, norm_gain, w_qkv, b_qkv, w_out):
    tok, d = x.shape
    ncache, groups, hd = k_cache.shape
    group = w_qkv.shape[1] // (groups * hd) - 2
    cp = lax.axis_index('cp')
    me = cp.astype(jnp.int32).reshape(1)
    bar = lax.optimization_barrier

    nper = 3
    wr = w_out.shape[0] // (4 * nper)
    w_parts = [lax.dynamic_slice(w_out, (cp * (nper * wr) + i * wr, 0), (wr, d)) for i in range(nper)]
    wy = [tp_send(p) for p in w_parts]

    cache = jnp.concatenate([k_cache.reshape(ncache, groups * hd), v_cache.reshape(ncache, groups * hd)], axis=1)
    caches = jnp.concatenate([cache] + [cp_send(cache, r) for r in (1, 2, 3)], axis=0)
    kc = caches[:, :groups * hd]
    vc = caches[:, groups * hd:].T

    half = rope_table.shape[1] // 2
    spread = jnp.dot(rope_table, spread_matrices(half, hd), precision=lax.Precision.HIGHEST)
    ce, se = spread[:, :hd], spread[:, hd:]
    bias = b_qkv.reshape(-1, 1, 2 * hd)

    h = norm(x, norm_gain)
    k, v, vt = project_kv(h, w_qkv, bias, ce, se, groups)
    ks, vs = cp_send(k, 1), cp_send(vt, 1)
    kx, vx = cp_send(k, 2), cp_send(vt, 2)
    q = project_q(h, w_qkv, bias, ce, se, groups)
    (q, kx, vx, wy[0]) = bar((q, kx, vx, wy[0]))
    kz, vz = cp_send(kx, 1), cp_send(vx, 1)
    pieces = [kc, vc, k, vt, ks, vs, kx, vx, kz, vz]

    wx, wd, wz = [None] * nper, [None] * nper, [None] * nper

    def forward(i):
        wx[i], wd[i] = cp_send(wy[i], 2), cp_send(wy[i], 1)

    def relay(i):
        wz[i] = cp_send(wx[i], 1)

    forward(0)
    outs, others = [], []
    for chunk in range(tok // QB):
        o = attend(chunk, me, q, pieces, group)
        if chunk == 1:
            (o, q, wy[1], wx[0]) = bar((o, q, wy[1], wx[0]))
            forward(1)
            relay(0)
        elif chunk == 3:
            (o, q, wy[2], wx[1]) = bar((o, q, wy[2], wx[1]))
            forward(2)
            relay(1)
        else:
            (o, q) = bar((o, q))
        outs.append(o)
        others.append(tp_send(o))

    partial = own_part(x, w_out, outs)
    (partial, wx[2]) = bar((partial, wx[2]))
    relay(2)
    ws = wy + wd + wx + wz
    y = None
    for chunk in range(tok // QB):
        y = other_part(chunk, me, others[chunk], partial, ws, y)
    return y, k.reshape(tok, groups, hd), v.reshape(tok, groups, hd)


def solution(mesh):
    row_spec = P(('dp', 'cp'), None)
    cache_spec = P(('dp', 'cp'), 'tp', None)
    return jax.shard_map(block, mesh=mesh, in_specs=(row_spec, cache_spec, cache_spec, row_spec, P(None), P(None, 'tp'), P('tp'), P('tp', None)), out_specs=(row_spec, cache_spec, cache_spec), check_vma=False)
```

```python
import functools

import jax
import jax.numpy as jnp
import numpy as np
from jax import lax
from jax.experimental import pallas as pl
from jax.experimental.pallas import tpu as pltpu
from jax.sharding import PartitionSpec as P


EPS = 1.5625e-07
MASK_VALUE = -1e30
F32 = jnp.float32
BF16 = jnp.bfloat16
LOG2E = 1.4426950408889634
HD = 128
VLIM = 60 * 1024 * 1024


def cost(flops, nbytes):
    return pl.CostEstimate(flops=int(flops), bytes_accessed=int(nbytes), transcendentals=0)


def dot(a, b):
    return jnp.dot(a, b, preferred_element_type=F32)


def norm_kernel(x_ref, g_ref, h_ref):
    x = x_ref[...].astype(F32)
    inv = lax.rsqrt(jnp.mean(x * x, axis=-1, keepdims=True) + EPS)
    h_ref[...] = (x * inv * g_ref[...].astype(F32)).astype(BF16)


def norm(x, g):
    rows, d = x.shape
    rb = 128
    return pl.pallas_call(
        norm_kernel,
        grid=(rows // rb,),
        in_specs=[pl.BlockSpec((rb, d), lambda i: (i, 0)), pl.BlockSpec((1, d), lambda i: (0, 0))],
        out_specs=pl.BlockSpec((rb, d), lambda i: (i, 0)),
        out_shape=jax.ShapeDtypeStruct((rows, d), BF16),
        cost_estimate=cost(rows * d * 80, rows * d * 4),
        name="norm",
    )(x, g.reshape(1, d))


def rotate(v, cos_e, sin_e):
    lane = lax.broadcasted_iota(jnp.int32, v.shape, 1)
    swapped = jnp.where(lane % 2 == 0, pltpu.roll(v, HD - 1, 1), pltpu.roll(v, 1, 1))
    return jnp.where(lane < HD // 2, v * cos_e + swapped * sin_e, v)


MB = 512


def kv_kernel(groups, h_ref, w_ref, b_ref, c_ref, s_ref, k_ref, v_ref, vt_ref, q_ref):
    bias = b_ref[0].astype(F32)
    first = pl.program_id(0) < groups

    @pl.loop(0, h_ref.shape[0] // MB)
    def _(m):
        r = pl.ds(pl.multiple_of(m * MB, MB), MB)
        a = dot(h_ref[r, :], w_ref[...]) + bias
        left = rotate(a[:, :HD], c_ref[r, :], s_ref[r, :]).astype(BF16)

        @pl.when(first)
        def _():
            k_ref[r, :] = left
            v = a[:, HD:].astype(BF16)
            v_ref[r, :] = v
            vt_ref[:, r] = v.T

        @pl.when(jnp.logical_not(first))
        def _():
            q_ref[r, :HD] = left
            q_ref[r, HD:] = rotate(a[:, HD:], c_ref[r, :], s_ref[r, :]).astype(BF16)


def q_kernel(h_ref, w_ref, b_ref, c_ref, s_ref, q_ref):
    bias = b_ref[0].astype(F32)

    @pl.loop(0, h_ref.shape[0] // MB)
    def _(m):
        r = pl.ds(pl.multiple_of(m * MB, MB), MB)
        a = dot(h_ref[r, :], w_ref[...]) + bias
        q_ref[r, :HD] = rotate(a[:, :HD], c_ref[r, :], s_ref[r, :]).astype(BF16)
        q_ref[r, HD:] = rotate(a[:, HD:], c_ref[r, :], s_ref[r, :]).astype(BF16)


def proj_specs(rows, d, col):
    whole = lambda i: (0, 0)
    return [
        pl.BlockSpec((rows, d), whole),
        pl.BlockSpec((d, 2 * HD), lambda i: (0, col(i))),
        pl.BlockSpec((1, 1, 2 * HD), lambda i: (col(i), 0, 0)),
        pl.BlockSpec((rows, HD), whole),
        pl.BlockSpec((rows, HD), whole),
    ]


def project_kv(h, w, b, ce, se, groups):
    rows, d = h.shape
    per = w.shape[1] // (2 * HD * groups)
    nq = per - 1
    steps = groups + nq
    col = lambda i: jnp.where(i < groups, i * per + nq, i - groups + (groups - 1) * per)
    at = lambda i: jnp.minimum(i, groups - 1)
    return pl.pallas_call(
        functools.partial(kv_kernel, groups),
        grid=(steps,),
        in_specs=proj_specs(rows, d, col),
        out_specs=[
            pl.BlockSpec((rows, HD), lambda i: (0, at(i))),
            pl.BlockSpec((rows, HD), lambda i: (0, at(i))),
            pl.BlockSpec((HD, rows), lambda i: (at(i), 0)),
            pl.BlockSpec((rows, 2 * HD), lambda i: (0, jnp.maximum(i - groups, 0))),
        ],
        out_shape=[
            jax.ShapeDtypeStruct((rows, groups * HD), BF16),
            jax.ShapeDtypeStruct((rows, groups * HD), BF16),
            jax.ShapeDtypeStruct((groups * HD, rows), BF16),
            jax.ShapeDtypeStruct((rows, nq * 2 * HD), BF16),
        ],
        compiler_params=pltpu.CompilerParams(vmem_limit_bytes=VLIM),
        cost_estimate=cost(2 * rows * d * steps * 2 * HD, d * steps * 4 * HD + rows * d * 2),
        name="project_kv",
    )(h, w, b, ce, se)


def project_q(h, w, b, ce, se, groups):
    rows, d = h.shape
    per = w.shape[1] // (2 * HD * groups)
    nq = per - 1
    steps = (groups - 1) * nq
    col = lambda i: (i // nq) * per + i % nq
    return pl.pallas_call(
        q_kernel,
        grid=(steps,),
        in_specs=proj_specs(rows, d, col),
        out_specs=pl.BlockSpec((rows, 2 * HD), lambda i: (0, i)),
        out_shape=jax.ShapeDtypeStruct((rows, steps * 2 * HD), BF16),
        compiler_params=pltpu.CompilerParams(vmem_limit_bytes=VLIM),
        cost_estimate=cost(2 * rows * d * steps * 2 * HD, d * steps * 4 * HD + rows * d * 2),
        name="project_q",
    )(h, w, b, ce, se)


QB = 256
KB = 1024


def attn_kernel(chunk, remotes, group, tok, me_ref, q_ref, ql_ref, *refs):
    nr = 1 if remotes else 0
    qr_ref = refs[0] if nr else None
    kc, vc, ko, vo, ks, vs, kx, vx, kz, vz = refs[nr:nr + 10]
    outs = refs[nr + 10:nr + 12 + nr]
    kbuf, vbuf, qt, sbuf, acc, mrun, lrun, obuf, sem = refs[nr + 12 + nr:]
    g = pl.program_id(0)
    groups = kbuf.shape[0]
    last = groups - 1
    me = me_ref[0]
    mirror = lax.bitwise_xor(me, 3)
    pieces = [(None, kc, vc), (0, ko, vo), (1, ks, vs), (2, kx, vx), (3, kz, vz)]

    def each_copy(gg, act):
        reach = jnp.maximum(me, mirror) if gg == last and remotes else me
        for rel, kp, vp in pieces:
            n = kp.shape[0]
            src = None if rel is None else lax.bitwise_xor(me, rel)
            at = 0 if rel is None else pl.multiple_of(kc.shape[0] + src * tok, tok)

            def go(kp=kp, vp=vp, n=n, at=at):
                act(pltpu.make_async_copy(kp.at[:, pl.ds(gg * HD, HD)], kbuf.at[gg, pl.ds(at, n), :], sem.at[gg]))
                act(pltpu.make_async_copy(vp.at[pl.ds(gg * HD, HD), :], vbuf.at[gg, :, pl.ds(at, n)], sem.at[gg]))

            if rel in (None, 0):
                go()
            else:
                pl.when(src <= reach)(go)

    @pl.when(g == 0)
    def _():
        for gg in range(groups):
            each_copy(gg, lambda c: c.start())

    for gg in range(groups):
        @pl.when(g == gg)
        def _(gg=gg):
            each_copy(gg, lambda c: c.wait())

    def load_q(ref):
        for h in range(group):
            qt[h] = ref[:, h * HD:(h + 1) * HD].T

    pl.when(g < last)(lambda: load_q(q_ref))
    pl.when(g == last)(lambda: load_q(ql_ref))
    if remotes:
        pl.when(g > last)(lambda: load_q(qr_ref))

    conv = LOG2E * HD ** -0.5
    kvg = jnp.minimum(g, last)

    def step(at, n, mask):
        k = kbuf[kvg, pl.ds(at, n), :]
        vt = vbuf[kvg, :, pl.ds(at, n)]
        sbuf[0, :n] = dot(k, qt[0])
        for h in range(group):
            if h + 1 < group:
                sbuf[(h + 1) % 2, :n] = dot(k, qt[h + 1])
            s = sbuf[h % 2, :n]
            if mask is not None:
                s = jnp.where(mask, s, MASK_VALUE)
            m_old = mrun[h]
            m_new = jnp.maximum(m_old, jnp.max(s, axis=0, keepdims=True))
            p = jnp.exp2(s * conv - m_new * conv)
            alpha = jnp.exp2((m_old - m_new) * conv)
            mrun[h] = m_new
            lrun[h] = lrun[h] * alpha + p.reshape(n // 8, 8, QB).sum(axis=0)
            acc[h] = acc[h] * alpha + dot(vt, p.astype(BF16))

    @pl.when((me < 2) | (g < last))
    def _():
        acc[...] = jnp.zeros_like(acc)
        lrun[...] = jnp.zeros_like(lrun)
        mrun[...] = jnp.full_like(mrun, MASK_VALUE)

        nfull = (kc.shape[0] + jnp.where(g > last, mirror, me) * tok) // KB

        @pl.loop(0, nfull)
        def _(kb):
            step(pl.multiple_of(kb * KB, KB), KB, None)

        def finish(c):
            tail = (c + 1) * QB
            key = lax.broadcasted_iota(jnp.int32, (tail, QB), 0)
            row = lax.broadcasted_iota(jnp.int32, (tail, QB), 1)
            step(pl.multiple_of(nfull * KB, KB), tail, key <= row + c * QB)

        others = [(i, c) for i, c in enumerate(remotes) if c != chunk]
        same = g <= last
        for i, c in enumerate(remotes):
            if c == chunk:
                same = same | (g == groups + i)
        if others:
            pl.when(same)(lambda: finish(chunk))
            for i, c in others:
                pl.when(g == groups + i)(lambda c=c: finish(c))
        else:
            finish(chunk)

        for h in range(group):
            total = jnp.sum(lrun[h], axis=0, keepdims=True)
            obuf[:, h * HD:(h + 1) * HD] = (acc[h] / total).T.astype(BF16)

        def put(ref):
            ref[...] = obuf[...]

        pl.when(g < last)(lambda: put(outs[0]))
        pl.when(g == last)(lambda: put(outs[1]))
        if remotes:
            pl.when(g > last)(lambda: put(outs[2]))


def attend(chunk, remotes, me, q, ql, qr, pieces, group):
    tok = q.shape[0]
    gw = group * HD
    groups = q.shape[1] // gw + 1
    last = groups - 1
    ncache = pieces[0].shape[0]
    total = ncache + 4 * tok
    anyspec = pl.BlockSpec(memory_space=pl.ANY)
    in_specs = [
        pl.BlockSpec((QB, gw), lambda g, me: (chunk, jnp.minimum(g, last - 1))),
        pl.BlockSpec((QB, gw), lambda g, me: (chunk, 0)),
    ]
    out_specs = [
        pl.BlockSpec((QB, gw), lambda g, me: (0, jnp.minimum(g, last - 1))),
        pl.BlockSpec((QB, gw), lambda g, me: (0, 0)),
    ]
    out_shape = [jax.ShapeDtypeStruct((QB, last * gw), BF16), jax.ShapeDtypeStruct((QB, gw), BF16)]
    args = [q, ql]
    if remotes:
        nrem = len(remotes)
        pos = lambda g: jnp.clip(g - groups, 0, nrem - 1)
        in_specs.append(pl.BlockSpec((QB, gw), lambda g, me: (remotes[0] + pos(g), 0)))
        out_specs.append(pl.BlockSpec((QB, gw), lambda g, me: (pos(g), 0)))
        out_shape.append(jax.ShapeDtypeStruct((QB * nrem, gw), BF16))
        args.append(qr)
    return pl.pallas_call(
        functools.partial(attn_kernel, chunk, remotes, group, tok),
        grid_spec=pltpu.PrefetchScalarGridSpec(
            num_scalar_prefetch=1,
            grid=(groups + len(remotes),),
            in_specs=in_specs + [anyspec] * 10,
            out_specs=out_specs,
            scratch_shapes=[
                pltpu.VMEM((groups, total, HD), BF16),
                pltpu.VMEM((groups, HD, total), BF16),
                pltpu.VMEM((group, HD, QB), BF16),
                pltpu.VMEM((2, KB, QB), F32),
                pltpu.VMEM((group, HD, QB), F32),
                pltpu.VMEM((group, 1, QB), F32),
                pltpu.VMEM((group, 8, QB), F32),
                pltpu.VMEM((QB, gw), BF16),
                pltpu.SemaphoreType.DMA((groups,)),
            ],
        ),
        out_shape=out_shape,
        compiler_params=pltpu.CompilerParams(vmem_limit_bytes=VLIM),
        cost_estimate=cost(40e9, 12e6),
    )(me, *args, *pieces)


def gather_rows(pieces, obuf, sem):
    @pl.when(pl.program_id(0) == 0)
    def _():
        copies = [pltpu.make_async_copy(c, obuf.at[pl.ds(r, c.shape[0]), pl.ds(w, c.shape[1])], sem.at[i])
                  for i, (r, w, c) in enumerate(pieces)]
        for c in copies:
            c.start()
        for c in copies:
            c.wait()


def layout(chunks):
    places = []
    for i, (a, b) in enumerate(chunks):
        places += [(i * a.shape[0], 0), (i * a.shape[0], a.shape[1])]
    return places


def own_kernel(places, x_ref, w_ref, *refs):
    n = len(places)
    y_ref, obuf, sem = refs[n:]
    gather_rows([(r, c, ref) for (r, c), ref in zip(places, refs[:n])], obuf, sem)

    @pl.loop(0, obuf.shape[0] // MB)
    def _(m):
        r = pl.ds(pl.multiple_of(m * MB, MB), MB)
        y_ref[r, :] = x_ref[r, :].astype(F32) + dot(obuf[r, :], w_ref[...])


def own_part(x, w, chunks):
    rows, d = x.shape
    inner = w.shape[0]
    nb = 512
    places = layout(chunks)
    return pl.pallas_call(
        functools.partial(own_kernel, places),
        grid=(d // nb,),
        in_specs=[
            pl.BlockSpec((rows, nb), lambda i: (0, i)),
            pl.BlockSpec((inner, nb), lambda i: (0, i)),
        ] + [pl.BlockSpec(memory_space=pl.ANY)] * len(places),
        out_specs=pl.BlockSpec((rows, nb), lambda i: (0, i)),
        out_shape=jax.ShapeDtypeStruct((rows, d), F32),
        scratch_shapes=[pltpu.VMEM((rows, inner), BF16), pltpu.SemaphoreType.DMA((len(places),))],
        compiler_params=pltpu.CompilerParams(vmem_limit_bytes=VLIM),
        cost_estimate=cost(2 * rows * inner * d, rows * d * 6 + inner * d * 2),
        name="own_part",
    )(x, w, *[p for c in chunks for p in c])


def other_kernel(nper, places, me_ref, a_ref, *refs):
    me = me_ref[0]
    nw, n = 4 * nper, len(places)
    ws, pieces = refs[:nw], refs[nw:nw + n]
    y_ref, obuf, sem = refs[-3:]
    gather_rows([(r, c, ref) for (r, c), ref in zip(places, pieces)], obuf, sem)
    wr = ws[0].shape[0]
    total = a_ref[...]
    for i in range(nw):
        quarter = lax.bitwise_xor(me, i // nper)
        at = pl.multiple_of(quarter * (nper * wr) + (i % nper) * wr, wr)
        total = total + dot(obuf[:, pl.ds(at, wr)], ws[i][...])
    y_ref[...] = total.astype(BF16)


def other_part(call, me, chunks, partial, ws, y):
    places = layout(chunks)
    rows = len(chunks) * chunks[0][0].shape[0]
    d = partial.shape[1]
    nb = 1024
    wr = ws[0].shape[0]
    extra = [] if y is None else [y]
    return pl.pallas_call(
        functools.partial(other_kernel, len(ws) // 4, places),
        grid_spec=pltpu.PrefetchScalarGridSpec(
            num_scalar_prefetch=1,
            grid=(d // nb,),
            in_specs=[pl.BlockSpec((rows, nb), lambda i, me: (call, i))]
            + [pl.BlockSpec((wr, nb), lambda i, me: (0, i))] * len(ws)
            + [pl.BlockSpec(memory_space=pl.ANY)] * (len(places) + len(extra)),
            out_specs=pl.BlockSpec((rows, nb), lambda i, me: (call, i)),
            scratch_shapes=[pltpu.VMEM((rows, wr * len(ws)), BF16), pltpu.SemaphoreType.DMA((len(places),))],
        ),
        out_shape=jax.ShapeDtypeStruct(partial.shape, BF16),
        input_output_aliases={} if y is None else {2 + len(ws) + len(places): 0},
        compiler_params=pltpu.CompilerParams(vmem_limit_bytes=VLIM),
        cost_estimate=cost(2 * rows * wr * len(ws) * d, rows * d * 6 + wr * len(ws) * d * 2),
    )(me, partial, *ws, *[p for c in chunks for p in c], *extra)


def cp_send(v, rel):
    return lax.ppermute(v, 'cp', [(i, i ^ rel) for i in range(4)])


def cp_move(v, pairs):
    return lax.ppermute(v, 'cp', pairs)


def tp_send(v):
    return lax.ppermute(v, 'tp', [(0, 1), (1, 0)])


def spread_matrices(half, hd):
    out = np.zeros((2 * half, 2 * hd), np.float32)
    for lane in range(2 * half):
        out[lane // 2, lane] = 1.0
        out[half + lane // 2, hd + lane] = 1.0 if lane % 2 else -1.0
    return out


def block(x, k_cache, v_cache, rope_table, norm_gain, w_qkv, b_qkv, w_out):
    tok, d = x.shape
    ncache, groups, hd = k_cache.shape
    group = w_qkv.shape[1] // (groups * hd) - 2
    cp = lax.axis_index('cp')
    me = cp.astype(jnp.int32).reshape(1)
    bar = lax.optimization_barrier

    nper = 3
    wr = w_out.shape[0] // (4 * nper)
    w_parts = [lax.dynamic_slice(w_out, (cp * (nper * wr) + i * wr, 0), (wr, d)) for i in range(nper)]
    wy = [tp_send(p) for p in w_parts]

    cache = jnp.concatenate([k_cache.reshape(ncache, groups * hd), v_cache.reshape(ncache, groups * hd)], axis=1)
    caches = jnp.concatenate([cache] + [cp_send(cache, r) for r in (1, 2, 3)], axis=0)
    kc = caches[:, :groups * hd]
    vc = caches[:, groups * hd:].T

    half = rope_table.shape[1] // 2
    spread = jnp.dot(rope_table, spread_matrices(half, hd), precision=lax.Precision.HIGHEST)
    ce, se = spread[:, :hd], spread[:, hd:]
    bias = b_qkv.reshape(-1, 1, 2 * hd)

    h = norm(x, norm_gain)
    k, v, vt, ql = project_kv(h, w_qkv, bias, ce, se, groups)
    ks, vs = cp_send(k, 1), cp_send(vt, 1)
    kx, vx = cp_send(k, 2), cp_send(vt, 2)
    qr = cp_move(ql, [(2, 1), (3, 0)])
    q = project_q(h, w_qkv, bias, ce, se, groups)
    (q, kx, vx, wy[0]) = bar((q, kx, vx, wy[0]))
    kz, vz = cp_send(kx, 1), cp_send(vx, 1)
    pieces = [kc, vc, k, vt, ks, vs, kx, vx, kz, vz]

    wx, wd, wz = [None] * nper, [None] * nper, [None] * nper

    def forward(i):
        wx[i], wd[i] = cp_send(wy[i], 2), cp_send(wy[i], 1)

    def relay(i):
        wz[i] = cp_send(wx[i], 1)

    forward(0)
    nchunk = tok // QB
    remotes = [(0,), (1,), (2, 3), ()]
    mine, theirs = [], []
    lasts, back, other_last = [None] * nchunk, [None] * nchunk, [None] * nchunk

    def settle(c):
        lasts[c] = jnp.where(cp >= 2, back[c], lasts[c])
        other_last[c] = tp_send(lasts[c])

    for chunk in range(nchunk):
        o, lasts[chunk], *rem = attend(chunk, remotes[chunk], me, q, ql, qr, pieces, group)
        if chunk == 0:
            (o, q) = bar((o, q))
        elif chunk == 1:
            (o, q, wy[1], wx[0], back[0]) = bar((o, q, wy[1], wx[0], back[0]))
            forward(1)
            relay(0)
            settle(0)
        elif chunk == 2:
            (o, q, back[1]) = bar((o, q, back[1]))
            settle(1)
        else:
            (o, q, wy[2], wx[1], back[2], back[3]) = bar((o, q, wy[2], wx[1], back[2], back[3]))
            settle(2)
            settle(3)
            forward(2)
            relay(1)
        if rem:
            got = cp_move(rem[0], [(0, 3), (1, 2)])
            for i, c in enumerate(remotes[chunk]):
                back[c] = got[i * QB:(i + 1) * QB]
        mine.append(o)
        theirs.append(tp_send(o))

    partial = own_part(x, w_out, list(zip(mine, lasts)))
    (partial, wx[2]) = bar((partial, wx[2]))
    relay(2)
    ws = wy + wd + wx + wz
    y = None
    for call in range(nchunk // 2):
        chunks = [(theirs[c], other_last[c]) for c in (2 * call, 2 * call + 1)]
        y = other_part(call, me, chunks, partial, ws, y)
    return y, k.reshape(tok, groups, hd), v.reshape(tok, groups, hd)


def solution(mesh):
    row_spec = P(('dp', 'cp'), None)
    cache_spec = P(('dp', 'cp'), 'tp', None)
    return jax.shard_map(block, mesh=mesh, in_specs=(row_spec, cache_spec, cache_spec, row_spec, P(None), P(None, 'tp'), P('tp'), P('tp', None)), out_specs=(row_spec, cache_spec, cache_spec), check_vma=False)
```

```python
import functools

import jax
import jax.numpy as jnp
import numpy as np
from jax import lax
from jax.experimental import pallas as pl
from jax.experimental.pallas import tpu as pltpu
from jax.sharding import PartitionSpec as P


EPS = 1.5625e-07
MASK_VALUE = -1e30
F32 = jnp.float32
BF16 = jnp.bfloat16
LOG2E = 1.4426950408889634
HD = 128
VLIM = 60 * 1024 * 1024


def cost(flops, nbytes):
    return pl.CostEstimate(flops=int(flops), bytes_accessed=int(nbytes), transcendentals=0)


def dot(a, b):
    return jnp.dot(a, b, preferred_element_type=F32)


def norm_kernel(x_ref, g_ref, h_ref):
    x = x_ref[...].astype(F32)
    inv = lax.rsqrt(jnp.mean(x * x, axis=-1, keepdims=True) + EPS)
    h_ref[...] = (x * inv * g_ref[...].astype(F32)).astype(BF16)


def norm(x, g):
    rows, d = x.shape
    rb = 128
    return pl.pallas_call(
        norm_kernel,
        grid=(rows // rb,),
        in_specs=[pl.BlockSpec((rb, d), lambda i: (i, 0)), pl.BlockSpec((1, d), lambda i: (0, 0))],
        out_specs=pl.BlockSpec((rb, d), lambda i: (i, 0)),
        out_shape=jax.ShapeDtypeStruct((rows, d), BF16),
        cost_estimate=cost(rows * d * 80, rows * d * 4),
        name="norm",
    )(x, g.reshape(1, d))


def rotate(v, cos_e, sin_e):
    lane = lax.broadcasted_iota(jnp.int32, v.shape, 1)
    swapped = jnp.where(lane % 2 == 0, pltpu.roll(v, HD - 1, 1), pltpu.roll(v, 1, 1))
    return jnp.where(lane < HD // 2, v * cos_e + swapped * sin_e, v)


MB = 512


def kv_kernel(groups, h_ref, w_ref, b_ref, c_ref, s_ref, kv_ref, v_ref, q_ref):
    bias = b_ref[0].astype(F32)
    i = pl.program_id(0)
    rows = h_ref.shape[0]

    @pl.loop(0, rows // MB)
    def _(m):
        r = pl.ds(pl.multiple_of(m * MB, MB), MB)
        a = dot(h_ref[r, :], w_ref[...]) + bias
        left = rotate(a[:, :HD], c_ref[r, :], s_ref[r, :]).astype(BF16)

        @pl.when(i < groups)
        def _():
            at = pl.multiple_of(jnp.minimum(i, groups - 1) * HD, HD)
            kv_ref[r, pl.ds(at, HD)] = left
            v = a[:, HD:].astype(BF16)
            v_ref[r, :] = v
            kv_ref[pl.ds(pl.multiple_of(rows + m * (groups * HD) + at, HD), HD), :] = v.T

        @pl.when(i >= groups)
        def _():
            q_ref[r, :HD] = left
            q_ref[r, HD:] = rotate(a[:, HD:], c_ref[r, :], s_ref[r, :]).astype(BF16)


def q_kernel(h_ref, w_ref, b_ref, c_ref, s_ref, q_ref):
    bias = b_ref[0].astype(F32)

    for m in range(h_ref.shape[0] // MB):
        r = pl.ds(m * MB, MB)
        a = dot(h_ref[r, :], w_ref[...]) + bias
        q_ref[r, :HD] = rotate(a[:, :HD], c_ref[r, :], s_ref[r, :]).astype(BF16)
        q_ref[r, HD:] = rotate(a[:, HD:], c_ref[r, :], s_ref[r, :]).astype(BF16)


def proj_specs(rows, d, col):
    whole = lambda i: (0, 0)
    return [
        pl.BlockSpec((rows, d), whole),
        pl.BlockSpec((d, 2 * HD), lambda i: (0, col(i))),
        pl.BlockSpec((1, 1, 2 * HD), lambda i: (col(i), 0, 0)),
        pl.BlockSpec((rows, HD), whole),
        pl.BlockSpec((rows, HD), whole),
    ]


def project_kv(h, w, b, ce, se, groups):
    assert groups * HD == MB
    rows, d = h.shape
    per = w.shape[1] // (2 * HD * groups)
    nq = per - 1
    steps = groups + nq
    col = lambda i: jnp.where(i < groups, i * per + nq, i - groups + (groups - 1) * per)
    at = lambda i: jnp.minimum(i, groups - 1)
    return pl.pallas_call(
        functools.partial(kv_kernel, groups),
        grid=(steps,),
        in_specs=proj_specs(rows, d, col),
        out_specs=[
            pl.BlockSpec((2 * rows, MB), lambda i: (0, 0)),
            pl.BlockSpec((rows, HD), lambda i: (0, at(i))),
            pl.BlockSpec((rows, 2 * HD), lambda i: (0, jnp.maximum(i - groups, 0))),
        ],
        out_shape=[
            jax.ShapeDtypeStruct((2 * rows, MB), BF16),
            jax.ShapeDtypeStruct((rows, groups * HD), BF16),
            jax.ShapeDtypeStruct((rows, nq * 2 * HD), BF16),
        ],
        compiler_params=pltpu.CompilerParams(vmem_limit_bytes=VLIM),
        cost_estimate=cost(2 * rows * d * steps * 2 * HD, d * steps * 4 * HD + rows * d * 2),
        name="project_kv",
    )(h, w, b, ce, se)


def project_q(h, w, b, ce, se, groups):
    rows, d = h.shape
    per = w.shape[1] // (2 * HD * groups)
    nq = per - 1
    steps = (groups - 1) * nq
    col = lambda i: (i // nq) * per + i % nq
    return pl.pallas_call(
        q_kernel,
        grid=(steps,),
        in_specs=proj_specs(rows, d, col),
        out_specs=pl.BlockSpec((rows, 2 * HD), lambda i: (0, i)),
        out_shape=jax.ShapeDtypeStruct((rows, steps * 2 * HD), BF16),
        compiler_params=pltpu.CompilerParams(vmem_limit_bytes=VLIM),
        cost_estimate=cost(2 * rows * d * steps * 2 * HD, d * steps * 4 * HD + rows * d * 2),
        name="project_q",
    )(h, w, b, ce, se)


def cache_kernel(k_ref, v_ref, out_ref):
    rows, groups, hd = k_ref.shape
    per = out_ref.shape[1] // rows
    for g in range(groups):
        out_ref[:rows, g * hd:(g + 1) * hd] = k_ref[:, g, :]
        top = rows + g // per * hd
        out_ref[top:top + hd, g % per * rows:(g % per + 1) * rows] = v_ref[:, g, :].T


def pack_cache(k, v):
    rows, groups, hd = k.shape
    return pl.pallas_call(
        cache_kernel,
        out_shape=jax.ShapeDtypeStruct((2 * rows, groups * hd), BF16),
        cost_estimate=cost(1e9, 1e6),
        name="pack_cache",
    )(k, v)


QB = 256
KB = 1024


def attn_kernel(chunk, remotes, group, tok, me_ref, q_ref, ql_ref, *refs):
    nr = 1 if remotes else 0
    qr_ref = refs[0] if nr else None
    pieces = refs[nr:nr + 4]
    caches = refs[nr + 4:nr + 8]
    outs = refs[nr + 8:nr + 10 + nr]
    kbuf, vbuf, qt, sbuf, acc, mrun, lrun, obuf, sem = refs[nr + 10 + nr:]
    g = pl.program_id(0)
    groups = kbuf.shape[0]
    last = groups - 1
    me = me_ref[0]
    mirror = lax.bitwise_xor(me, 3)
    nc = caches[0].shape[0] // 2
    ncache = 4 * nc
    per = caches[0].shape[1] // nc

    def each_copy(gg, act):
        reach = jnp.maximum(me, mirror) if gg == last and remotes else me
        cols = pl.ds(gg * HD, HD)

        def k_copy(ref, n, at):
            act(pltpu.make_async_copy(ref.at[pl.ds(0, n), cols], kbuf.at[gg, pl.ds(at, n), :], sem.at[gg]))

        def v_copy(ref, top, left, n, at):
            act(pltpu.make_async_copy(ref.at[pl.ds(top, HD), pl.ds(left, n)], vbuf.at[gg, :, pl.ds(at, n)], sem.at[gg]))

        for i, ref in enumerate(caches):
            k_copy(ref, nc, i * nc)
            v_copy(ref, nc + gg // per * HD, gg % per * nc, nc, i * nc)
        for rel, ref in enumerate(pieces):
            src = lax.bitwise_xor(me, rel)
            at = pl.multiple_of(ncache + src * tok, tok)

            def go(ref=ref, at=at):
                k_copy(ref, tok, at)
                for m in range(tok // MB):
                    v_copy(ref, tok + m * groups * HD + gg * HD, 0, MB, pl.multiple_of(at + m * MB, MB))

            if rel == 0:
                go()
            else:
                pl.when(src <= reach)(go)

    @pl.when(g == 0)
    def _():
        for gg in range(groups):
            each_copy(gg, lambda c: c.start())

    for gg in range(groups):
        @pl.when(g == gg)
        def _(gg=gg):
            each_copy(gg, lambda c: c.wait())

    def load_q(ref):
        for h in range(group):
            qt[h] = ref[:, h * HD:(h + 1) * HD].T

    pl.when(g < last)(lambda: load_q(q_ref))
    pl.when(g == last)(lambda: load_q(ql_ref))
    if remotes:
        pl.when(g > last)(lambda: load_q(qr_ref))

    conv = LOG2E * HD ** -0.5
    kvg = jnp.minimum(g, last)

    def keys(at, n):
        return kbuf[kvg, pl.ds(at, n), :]

    def step(at, n, mask, ahead):
        k = keys(at, n)
        vt = vbuf[kvg, :, pl.ds(at, n)]
        for h in range(group):
            if h + 1 < group:
                sbuf[(h + 1) % 2, :n] = dot(k, qt[h + 1])
            elif ahead is not None:
                sbuf[(h + 1) % 2] = dot(keys(ahead, KB), qt[0])
            s = sbuf[h % 2, :n]
            if mask is not None:
                s = jnp.where(mask, s, MASK_VALUE)
            m_old = mrun[h]
            m_new = jnp.maximum(m_old, jnp.max(s, axis=0, keepdims=True))
            p = jnp.exp2(s * conv - m_new * conv)
            alpha = jnp.exp2((m_old - m_new) * conv)
            mrun[h] = m_new
            lrun[h] = lrun[h] * alpha + p.reshape(n // 8, 8, QB).sum(axis=0)
            acc[h] = acc[h] * alpha + dot(vt, p.astype(BF16))

    @pl.when((me < 2) | (g < last))
    def _():
        acc[...] = jnp.zeros_like(acc)
        lrun[...] = jnp.zeros_like(lrun)
        mrun[...] = jnp.full_like(mrun, MASK_VALUE)

        nfull = (ncache + jnp.where(g > last, mirror, me) * tok) // KB

        sbuf[0] = dot(keys(0, KB), qt[0])

        @pl.loop(0, nfull)
        def _(kb):
            step(pl.multiple_of(kb * KB, KB), KB, None, pl.multiple_of((kb + 1) * KB, KB))

        def finish(c):
            tail = (c + 1) * QB
            key = lax.broadcasted_iota(jnp.int32, (tail, QB), 0)
            row = lax.broadcasted_iota(jnp.int32, (tail, QB), 1)
            step(pl.multiple_of(nfull * KB, KB), tail, key <= row + c * QB, None)

        others = [(i, c) for i, c in enumerate(remotes) if c != chunk]
        same = g <= last
        for i, c in enumerate(remotes):
            if c == chunk:
                same = same | (g == groups + i)
        if others:
            pl.when(same)(lambda: finish(chunk))
            for i, c in others:
                pl.when(g == groups + i)(lambda c=c: finish(c))
        else:
            finish(chunk)

        for h in range(group):
            total = jnp.sum(lrun[h], axis=0, keepdims=True)
            obuf[:, h * HD:(h + 1) * HD] = (acc[h] / total).T.astype(BF16)

        def put(ref):
            ref[...] = obuf[...]

        pl.when(g < last)(lambda: put(outs[0]))
        pl.when(g == last)(lambda: put(outs[1]))
        if remotes:
            pl.when(g > last)(lambda: put(outs[2]))


def attend(chunk, remotes, me, q, ql, qr, pieces, caches, group):
    tok = q.shape[0]
    gw = group * HD
    groups = q.shape[1] // gw + 1
    last = groups - 1
    total = 2 * caches[0].shape[0] + 4 * tok
    assert group % 2 == 0 and tok == KB and 2 * caches[0].shape[0] % KB == 0
    anyspec = pl.BlockSpec(memory_space=pl.ANY)
    in_specs = [
        pl.BlockSpec((QB, gw), lambda g, me: (chunk, jnp.minimum(g, last - 1))),
        pl.BlockSpec((QB, gw), lambda g, me: (chunk, 0)),
    ]
    out_specs = [
        pl.BlockSpec((QB, gw), lambda g, me: (0, jnp.minimum(g, last - 1))),
        pl.BlockSpec((QB, gw), lambda g, me: (0, 0)),
    ]
    out_shape = [jax.ShapeDtypeStruct((QB, last * gw), BF16), jax.ShapeDtypeStruct((QB, gw), BF16)]
    args = [q, ql]
    if remotes:
        nrem = len(remotes)
        pos = lambda g: jnp.clip(g - groups, 0, nrem - 1)
        in_specs.append(pl.BlockSpec((QB, gw), lambda g, me: (remotes[0] + pos(g), 0)))
        out_specs.append(pl.BlockSpec((QB, gw), lambda g, me: (pos(g), 0)))
        out_shape.append(jax.ShapeDtypeStruct((QB * nrem, gw), BF16))
        args.append(qr)
    return pl.pallas_call(
        functools.partial(attn_kernel, chunk, remotes, group, tok),
        grid_spec=pltpu.PrefetchScalarGridSpec(
            num_scalar_prefetch=1,
            grid=(groups + len(remotes),),
            in_specs=in_specs + [anyspec] * 8,
            out_specs=out_specs,
            scratch_shapes=[
                pltpu.VMEM((groups, total, HD), BF16),
                pltpu.VMEM((groups, HD, total), BF16),
                pltpu.VMEM((group, HD, QB), BF16),
                pltpu.VMEM((2, KB, QB), F32),
                pltpu.VMEM((group, HD, QB), F32),
                pltpu.VMEM((group, 1, QB), F32),
                pltpu.VMEM((group, 8, QB), F32),
                pltpu.VMEM((QB, gw), BF16),
                pltpu.SemaphoreType.DMA((groups,)),
            ],
        ),
        out_shape=out_shape,
        compiler_params=pltpu.CompilerParams(vmem_limit_bytes=VLIM),
        cost_estimate=cost(40e9, 12e6),
    )(me, *args, *pieces, *caches)


def gather_rows(pieces, obuf, sem):
    @pl.when(pl.program_id(0) == 0)
    def _():
        copies = [pltpu.make_async_copy(c, obuf.at[pl.ds(r, c.shape[0]), pl.ds(w, c.shape[1])], sem.at[i])
                  for i, (r, w, c) in enumerate(pieces)]
        for c in copies:
            c.start()
        for c in copies:
            c.wait()


def layout(chunks):
    places = []
    for i, (a, b) in enumerate(chunks):
        places += [(i * a.shape[0], 0), (i * a.shape[0], a.shape[1])]
    return places


def own_kernel(places, x_ref, w_ref, *refs):
    n = len(places)
    y_ref, obuf, sem = refs[n:]
    gather_rows([(r, c, ref) for (r, c), ref in zip(places, refs[:n])], obuf, sem)

    @pl.loop(0, obuf.shape[0] // MB)
    def _(m):
        r = pl.ds(pl.multiple_of(m * MB, MB), MB)
        y_ref[r, :] = x_ref[r, :].astype(F32) + dot(obuf[r, :], w_ref[...])


def own_part(x, w, chunks):
    rows, d = x.shape
    inner = w.shape[0]
    nb = 512
    places = layout(chunks)
    return pl.pallas_call(
        functools.partial(own_kernel, places),
        grid=(d // nb,),
        in_specs=[
            pl.BlockSpec((rows, nb), lambda i: (0, i)),
            pl.BlockSpec((inner, nb), lambda i: (0, i)),
        ] + [pl.BlockSpec(memory_space=pl.ANY)] * len(places),
        out_specs=pl.BlockSpec((rows, nb), lambda i: (0, i)),
        out_shape=jax.ShapeDtypeStruct((rows, d), F32),
        scratch_shapes=[pltpu.VMEM((rows, inner), BF16), pltpu.SemaphoreType.DMA((len(places),))],
        compiler_params=pltpu.CompilerParams(vmem_limit_bytes=VLIM),
        cost_estimate=cost(2 * rows * inner * d, rows * d * 6 + inner * d * 2),
        name="own_part",
    )(x, w, *[p for c in chunks for p in c])


def other_kernel(nper, places, me_ref, a_ref, *refs):
    me = me_ref[0]
    nw, n = 4 * nper, len(places)
    ws, pieces = refs[:nw], refs[nw:nw + n]
    y_ref, obuf, sem = refs[-3:]
    gather_rows([(r, c, ref) for (r, c), ref in zip(places, pieces)], obuf, sem)
    wr = ws[0].shape[0]

    @pl.loop(0, obuf.shape[0] // MB)
    def _(m):
        r = pl.ds(pl.multiple_of(m * MB, MB), MB)
        total = a_ref[r, :]
        for i in range(nw):
            quarter = lax.bitwise_xor(me, i // nper)
            at = pl.multiple_of(quarter * (nper * wr) + (i % nper) * wr, wr)
            total = total + dot(obuf[r, pl.ds(at, wr)], ws[i][...])
        y_ref[r, :] = total.astype(BF16)


def other_part(call, me, chunks, partial, ws, y):
    places = layout(chunks)
    rows = len(chunks) * chunks[0][0].shape[0]
    d = partial.shape[1]
    nb = 512
    wr = ws[0].shape[0]
    extra = [] if y is None else [y]
    return pl.pallas_call(
        functools.partial(other_kernel, len(ws) // 4, places),
        grid_spec=pltpu.PrefetchScalarGridSpec(
            num_scalar_prefetch=1,
            grid=(d // nb,),
            in_specs=[pl.BlockSpec((rows, nb), lambda i, me: (call, i))]
            + [pl.BlockSpec((wr, nb), lambda i, me: (0, i))] * len(ws)
            + [pl.BlockSpec(memory_space=pl.ANY)] * (len(places) + len(extra)),
            out_specs=pl.BlockSpec((rows, nb), lambda i, me: (call, i)),
            scratch_shapes=[pltpu.VMEM((rows, wr * len(ws)), BF16), pltpu.SemaphoreType.DMA((len(places),))],
        ),
        out_shape=jax.ShapeDtypeStruct(partial.shape, BF16),
        input_output_aliases={} if y is None else {2 + len(ws) + len(places): 0},
        compiler_params=pltpu.CompilerParams(vmem_limit_bytes=VLIM),
        cost_estimate=cost(2 * rows * wr * len(ws) * d, rows * d * 6 + wr * len(ws) * d * 2),
    )(me, partial, *ws, *[p for c in chunks for p in c], *extra)


def cp_send(v, rel):
    return lax.ppermute(v, 'cp', [(i, i ^ rel) for i in range(4)])


def cp_move(v, pairs):
    return lax.ppermute(v, 'cp', pairs)


def tp_send(v):
    return lax.ppermute(v, 'tp', [(0, 1), (1, 0)])


def spread_matrices(half, hd):
    out = np.zeros((2 * half, 2 * hd), np.float32)
    for lane in range(2 * half):
        out[lane // 2, lane] = 1.0
        out[half + lane // 2, hd + lane] = 1.0 if lane % 2 else -1.0
    return out


def block(x, k_cache, v_cache, rope_table, norm_gain, w_qkv, b_qkv, w_out):
    tok, d = x.shape
    _, groups, hd = k_cache.shape
    group = w_qkv.shape[1] // (groups * hd) - 2
    cp = lax.axis_index('cp')
    me = cp.astype(jnp.int32).reshape(1)
    bar = lax.optimization_barrier

    nper = 3
    wr = w_out.shape[0] // (4 * nper)
    w_parts = [lax.dynamic_slice(w_out, (cp * (nper * wr) + i * wr, 0), (wr, d)) for i in range(nper)]
    wy = [tp_send(p) for p in w_parts]

    cache = pack_cache(k_cache, v_cache)
    caches = [cache] + [cp_send(cache, r) for r in (1, 2, 3)]

    half = rope_table.shape[1] // 2
    spread = jnp.dot(rope_table, spread_matrices(half, hd), precision=lax.Precision.HIGHEST)
    ce, se = spread[:, :hd], spread[:, hd:]
    bias = b_qkv.reshape(-1, 1, 2 * hd)

    h = norm(x, norm_gain)
    kv, v, ql = project_kv(h, w_qkv, bias, ce, se, groups)
    kvx = cp_send(kv, 2)
    kvs = cp_send(kv, 1)
    qr = cp_move(ql, [(2, 1), (3, 0)])
    q = project_q(h, w_qkv, bias, ce, se, groups)
    (q, kvx, wy[0]) = bar((q, kvx, wy[0]))
    pieces = [kv, kvs, kvx, cp_send(kvx, 1)]

    wx, wd, wz = [None] * nper, [None] * nper, [None] * nper

    def forward(i):
        wx[i], wd[i] = cp_send(wy[i], 2), cp_send(wy[i], 1)

    def relay(i):
        wz[i] = cp_send(wx[i], 1)

    forward(0)
    nchunk = tok // QB
    remotes = [(), (0, 1), (2, 3), ()]
    mine, theirs = [], []
    lasts, back, other_last = [None] * nchunk, [None] * nchunk, [None] * nchunk

    def settle(c):
        lasts[c] = jnp.where(cp >= 2, back[c], lasts[c])
        other_last[c] = tp_send(lasts[c])

    for chunk in range(nchunk):
        o, lasts[chunk], *rem = attend(chunk, remotes[chunk], me, q, ql, qr, pieces, caches, group)
        if chunk == 0:
            (o, q, wy[1]) = bar((o, q, wy[1]))
            forward(1)
        elif chunk == 1:
            (o, q, wy[2], wx[0]) = bar((o, q, wy[2], wx[0]))
            forward(2)
            relay(0)
        elif chunk == 2:
            (o, q, back[0], back[1]) = bar((o, q, back[0], back[1]))
            settle(0)
            settle(1)
        else:
            (o, q, wx[1], back[2], back[3]) = bar((o, q, wx[1], back[2], back[3]))
            settle(2)
            settle(3)
            relay(1)
        if rem:
            got = cp_move(rem[0], [(0, 3), (1, 2)])
            for i, c in enumerate(remotes[chunk]):
                back[c] = got[i * QB:(i + 1) * QB]
        mine.append(o)
        theirs.append(tp_send(o))

    partial = own_part(x, w_out, list(zip(mine, lasts)))
    (partial, wx[2]) = bar((partial, wx[2]))
    relay(2)
    ws = wy + wd + wx + wz
    y = other_part(0, me, list(zip(theirs, other_last)), partial, ws, None)
    k = kv[:tok]
    return y, k.reshape(tok, groups, hd), v.reshape(tok, groups, hd)


def solution(mesh):
    row_spec = P(('dp', 'cp'), None)
    cache_spec = P(('dp', 'cp'), 'tp', None)
    return jax.shard_map(block, mesh=mesh, in_specs=(row_spec, cache_spec, cache_spec, row_spec, P(None), P(None, 'tp'), P('tp'), P('tp', None)), out_specs=(row_spec, cache_spec, cache_spec), check_vma=False)
```
